32 devices in a mesh: stage: 4 (over z), expert: 8 (over y, x, core).
Axes of the slice: x: 2, y: 2, z: 4, core: 2. Of those that a mesh axis runs over, the one named last changes fastest.
Arguments:
- w_gate: bfloat16 [12, 8, 1024, 512], P('stage', 'expert')
- w_up: bfloat16 [12, 8, 1024, 512], P('stage', 'expert')
- w_down: bfloat16 [12, 8, 512, 1024], P('stage', 'expert')
- hot_units: int32 [1], replicated
- slot_map: int32 [32, 2], replicated
Outputs:
- output 1: bfloat16 [12, 96, 1024, 256], P(None, ('stage', 'expert'))
- output 2: bfloat16 [12, 96, 128, 1024], P(None, ('stage', 'expert'))
All inputs are finite; a program needn't handle non-finite values.
Results may differ from the reference program's by a relative error of at most 0.001.
Values are sent between devices in bfloat16 or wider.
A program may use at most 1 GiB of HBM per device.

```python
import jax
import jax.numpy as jnp

LAYERS = 12
EXPERTS = 8
D_MODEL = 1024
FF_EXPERT = 512
DEVICES_FLAT = 32
HOT_UNITS = 1
EXTRA_SLOTS = 2

SPLIT_COUNT = max(DEVICES_FLAT // EXPERTS, 1)
UNITS_DEV = max(EXPERTS // DEVICES_FLAT, 1)
FF_DEV = FF_EXPERT // SPLIT_COUNT
UNIT_COUNT = EXPERTS * SPLIT_COUNT
SLOTS_DEV = UNITS_DEV + EXTRA_SLOTS
REPLICAS = 3 * DEVICES_FLAT // 2


def setup_inputs(seed: int = 0) -> dict:
    base_key = jax.random.key(seed)
    key_gate, key_up, key_down, key_hot, key_slot = jax.random.split(base_key, 5)
    gate_shape = (LAYERS, EXPERTS, D_MODEL, FF_EXPERT)
    down_shape = (LAYERS, EXPERTS, FF_EXPERT, D_MODEL)
    w_gate = (jax.random.normal(key_gate, gate_shape, jnp.float32) * D_MODEL ** -0.5).astype(jnp.bfloat16)
    w_up = (jax.random.normal(key_up, gate_shape, jnp.float32) * D_MODEL ** -0.5).astype(jnp.bfloat16)
    w_down = (jax.random.normal(key_down, down_shape, jnp.float32) * FF_EXPERT ** -0.5).astype(jnp.bfloat16)
    hot_units = jax.random.permutation(key_hot, UNIT_COUNT)[:HOT_UNITS].astype(jnp.int32)
    slot_order = jax.random.permutation(key_slot, DEVICES_FLAT * EXTRA_SLOTS)
    slot_map = jnp.where(slot_order < REPLICAS, slot_order % HOT_UNITS, -1).astype(jnp.int32).reshape(DEVICES_FLAT, EXTRA_SLOTS)
    return {'w_gate': w_gate, 'w_up': w_up, 'w_down': w_down, 'hot_units': hot_units, 'slot_map': slot_map}


def reference(w_gate, w_up, w_down, hot_units, slot_map):
    gate_parts = w_gate.reshape(LAYERS, EXPERTS, D_MODEL, SPLIT_COUNT, FF_DEV)
    up_parts = w_up.reshape(LAYERS, EXPERTS, D_MODEL, SPLIT_COUNT, FF_DEV)
    fused_units = jnp.concatenate([gate_parts, up_parts], axis=-1).transpose(0, 1, 3, 2, 4).reshape(LAYERS, UNIT_COUNT, D_MODEL, 2 * FF_DEV)
    down_units = w_down.reshape(LAYERS, UNIT_COUNT, FF_DEV, D_MODEL)
    slot_used = slot_map >= 0
    extra_ids = jnp.where(slot_used, hot_units[jnp.maximum(slot_map, 0)], 0).reshape(-1)
    keep_mask = slot_used.reshape(1, DEVICES_FLAT, EXTRA_SLOTS, 1, 1)
    fused_extra = jnp.where(keep_mask, jnp.take(fused_units, extra_ids, axis=1).reshape(LAYERS, DEVICES_FLAT, EXTRA_SLOTS, D_MODEL, 2 * FF_DEV), 0)
    down_extra = jnp.where(keep_mask, jnp.take(down_units, extra_ids, axis=1).reshape(LAYERS, DEVICES_FLAT, EXTRA_SLOTS, FF_DEV, D_MODEL), 0)
    fused_home = fused_units.reshape(LAYERS, DEVICES_FLAT, UNITS_DEV, D_MODEL, 2 * FF_DEV)
    down_home = down_units.reshape(LAYERS, DEVICES_FLAT, UNITS_DEV, FF_DEV, D_MODEL)
    w13 = jnp.concatenate([fused_home, fused_extra], axis=2).reshape(LAYERS, DEVICES_FLAT * SLOTS_DEV, D_MODEL, 2 * FF_DEV)
    w_down_out = jnp.concatenate([down_home, down_extra], axis=2).reshape(LAYERS, DEVICES_FLAT * SLOTS_DEV, FF_DEV, D_MODEL)
    return w13, w_down_out
```

```python
import functools

import jax
import jax.numpy as jnp
from jax import lax
from jax.experimental import pallas as pl
from jax.experimental.pallas import tpu as pltpu
from jax.sharding import PartitionSpec as P

MESH = pl.DeviceIdType.MESH
BF16 = jnp.bfloat16


def exchange_kernel(dims, hot_ref, gate, up, down, home13, homed, hot13, hotd,
                    part_g, part_u, part_d, cand13, candd, rel13, reld, got13, gotd, sel13, seld,
                    s_own, s_p1, s_z, s_hs, s_hz, s_hp,
                    r_rel, r_home, r_hs, r_hz, r_hp, l_own, l_rel, l_part, l_hot):
    nl, dm, ff = dims
    z = lax.axis_index('stage')
    j = lax.axis_index('expert')
    y, x, c = j // 4, (j // 2) % 2, j % 2
    zt = j // 2
    r8 = dm // 8
    d8 = ff // 8

    def dev(zz, yy, xx, cc):
        return (zz, 4 * yy + 2 * xx + cc)

    def rdma(src, dst, ss, rs, to):
        return pltpu.make_async_remote_copy(src_ref=src, dst_ref=dst, send_sem=ss, recv_sem=rs,
                                            device_id=to, device_id_type=MESH)

    def landed(ref, sem):
        rdma(ref, ref, sem, sem, (z, j)).wait_recv()

    def cols(k):
        return pl.ds(pl.multiple_of(k * ff, ff), ff)

    def pieces(t, k, dst13, dstd):
        return ((gate.at[t, 0, :, cols(k)], dst13.at[:, pl.ds(0, ff)]),
                (up.at[t, 0, :, cols(k)], dst13.at[:, pl.ds(ff, ff)]),
                (down.at[t, 0, cols(k), :], dstd))

    def own(t, do_local, do_remote):
        lay = nl * z + t
        for kc in range(2):
            k = 2 * x + kc
            todo = pieces(t, k, home13.at[lay], homed.at[lay])
            stays = jnp.logical_and(z == zt, c == kc)

            @pl.when(jnp.logical_and(c == y, stays))
            def _():
                for a, (src, dst) in enumerate(todo):
                    do_local(pltpu.make_async_copy(src, dst, l_own.at[t, a]))

            @pl.when(jnp.logical_and(c == y, jnp.logical_not(stays)))
            def _():
                for a, (src, dst) in enumerate(todo):
                    do_remote(rdma(src, dst, s_own.at[kc, t, a], r_home.at[lay, a // 2], dev(zt, y, x, kc)))

    def p1(t, do):
        def to(dx, m, slot):
            xx = (x + dx) % 2
            for kc in range(2):
                for a, (src, dst) in enumerate(pieces(t, 2 * xx + kc, rel13.at[m, t], reld.at[m, t])):
                    do(rdma(src, dst, s_p1.at[slot, kc, t, a], r_rel.at[m, t, a // 2], dev(z, c, xx, kc)))

        @pl.when(c == y)
        def _():
            to(1, 0, 0)

        @pl.when(c != y)
        def _():
            to(0, 1, 0)
            to(1, 2, 1)

    relays = ((2 * y + 1 - x), (2 * (1 - y) + x), (2 * (1 - y) + 1 - x))

    def zsend(t, wait, do_local, do_remote):
        lay = nl * z + t
        for m in range(3):
            zm = relays[m]
            src = (rel13.at[m, t], reld.at[m, t])
            dst = (home13.at[lay], homed.at[lay])
            if wait:
                for a in range(2):
                    landed(src[a], r_rel.at[m, t, a])

            @pl.when(zm == z)
            def _():
                for a in range(2):
                    do_local(pltpu.make_async_copy(src[a], dst[a], l_rel.at[t, a]))

            @pl.when(zm != z)
            def _():
                for a in range(2):
                    do_remote(rdma(src[a], dst[a], s_z.at[m, t, a], r_home.at[lay, a], (zm, j)))

    start = lambda cp: cp.start()
    wait_send = lambda cp: cp.wait_send()
    wait = lambda cp: cp.wait()
    skip = lambda cp: None

    def part_loads():
        for k in range(4):
            yield pltpu.make_async_copy(gate.at[:, 0, :, pl.ds(k * ff, ff)], part_g.at[k], l_part.at[k, 0])
            yield pltpu.make_async_copy(up.at[:, 0, :, pl.ds(k * ff, ff)], part_u.at[k], l_part.at[k, 1])
            yield pltpu.make_async_copy(down.at[:, 0, pl.ds(k * ff, ff), :], part_d.at[k], l_part.at[k, 2])

    def rows13(q):
        return pl.ds(pl.multiple_of(q * r8, r8), r8)

    def rowsd(q):
        return pl.ds(pl.multiple_of(q * d8, d8), d8)

    def scatter_local():
        yield pltpu.make_async_copy(cand13.at[:, rows13(j), :], got13.at[j], l_hot.at[0])
        yield pltpu.make_async_copy(candd.at[:, rowsd(j), :], gotd.at[j], l_hot.at[1])

    def scatter():
        for d in range(1, 8):
            q = (j + d) % 8
            yield rdma(cand13.at[:, rows13(q), :], got13.at[j], s_hs.at[d, 0], r_hs.at[j, 0], (z, q))
            yield rdma(candd.at[:, rowsd(q), :], gotd.at[j], s_hs.at[d, 1], r_hs.at[j, 1], (z, q))

    def hot_piece(zz, q):
        ls = pl.ds(nl * zz, nl)
        return hot13.at[ls, rows13(q), :], hotd.at[ls, rowsd(q), :]

    def hot_rows(q):
        return hot13.at[:, rows13(q), :], hotd.at[:, rowsd(q), :]

    z1 = z + 1 - 2 * (z % 2)
    zc = 3 - z
    zf = 3 - z1

    def sel_local():
        p13, pd = hot_piece(z, j)
        yield pltpu.make_async_copy(sel13, p13, l_hot.at[2])
        yield pltpu.make_async_copy(seld, pd, l_hot.at[3])

    def along_z():
        p13, pd = hot_piece(z, j)
        for i, to in enumerate((zc, z1)):
            yield rdma(sel13, p13, s_hz.at[i, 0], r_hz.at[z, 0], (to, j))
            yield rdma(seld, pd, s_hz.at[i, 1], r_hz.at[z, 1], (to, j))

    def forward_z():
        p13, pd = hot_piece(zc, j)
        yield rdma(p13, p13, s_hz.at[2, 0], r_hz.at[zc, 0], (z1, j))
        yield rdma(pd, pd, s_hz.at[2, 1], r_hz.at[zc, 1], (z1, j))

    def hot_z_landed(zz):
        for a, ref in enumerate(hot_piece(zz, j)):
            landed(ref, r_hz.at[zz, a])

    same_core = ((y, 1 - x), (1 - y, x), (1 - y, 1 - x))

    def gather():
        p13, pd = hot_rows(j)
        for i, (yy, xx) in enumerate(same_core):
            yield rdma(p13, p13, s_hp.at[i, 0], r_hp.at[j, 0], dev(z, yy, xx, c))
            yield rdma(pd, pd, s_hp.at[i, 1], r_hp.at[j, 1], dev(z, yy, xx, c))
        yield rdma(p13, p13, s_hp.at[3, 0], r_hp.at[j, 0], dev(z, y, x, 1 - c))
        yield rdma(pd, pd, s_hp.at[3, 1], r_hp.at[j, 1], dev(z, y, x, 1 - c))

    def hot_rows_landed(q):
        for a, ref in enumerate(hot_rows(q)):
            landed(ref, r_hp.at[q, a])

    def to_sibling(i):
        yy, xx = same_core[i]
        q = 4 * yy + 2 * xx + c
        p13, pd = hot_rows(q)
        yield rdma(p13, p13, s_hp.at[4 + i, 0], r_hp.at[q, 0], dev(z, y, x, 1 - c))
        yield rdma(pd, pd, s_hp.at[4 + i, 1], r_hp.at[q, 1], dev(z, y, x, 1 - c))

    own(0, start, start)
    p1(0, start)
    for cp in part_loads():
        cp.start()
    for cp in part_loads():
        cp.wait()
    kh = lax.rem(hot_ref[0], 4)
    eh = lax.div(hot_ref[0], 4)

    def build(i, carry):
        t, b = i // 8, i % 8
        rr = pl.ds(pl.multiple_of(b * r8, r8), r8)
        rd = pl.ds(pl.multiple_of(b * d8, d8), d8)
        cand13[t, rr, 0:ff] = part_g[kh, t, rr, :]
        cand13[t, rr, ff:2 * ff] = part_u[kh, t, rr, :]
        candd[t, rd, :] = part_d[kh, t, rd, :]
        return carry

    lax.fori_loop(0, nl * 8, build, 0)
    p1(1, start)
    for cp in scatter_local():
        cp.start()
    for cp in scatter():
        cp.start()
    p1(2, start)

    zsend(0, True, start, start)
    for cp in scatter_local():
        cp.wait()
    for d in range(1, 8):
        q = (j + d) % 8
        landed(got13.at[q], r_hs.at[q, 0])
        landed(gotd.at[q], r_hs.at[q, 1])
    sel13[...] = got13[eh]
    seld[...] = gotd[eh]
    own(1, start, start)
    for cp in sel_local():
        cp.start()
    for cp in along_z():
        cp.start()
    zsend(1, True, start, start)
    hot_z_landed(zc)
    for cp in forward_z():
        cp.start()
    own(2, start, start)
    zsend(2, True, start, start)

    for cp in sel_local():
        cp.wait()
    hot_z_landed(z1)
    hot_z_landed(zf)
    for cp in gather():
        cp.start()
    for i in range(3):
        yy, xx = same_core[i]
        hot_rows_landed(4 * yy + 2 * xx + c)
        for cp in to_sibling(i):
            cp.start()

    for yy in range(2):
        for xx in range(2):
            hot_rows_landed(4 * yy + 2 * xx + 1 - c)
    for zz in range(4):
        for t in range(nl):
            lay = nl * zz + t
            away = z != zz
            sib = jnp.logical_and(z == zt, c != y)

            @pl.when(jnp.logical_or(away, sib))
            def _():
                landed(home13.at[lay], r_home.at[lay, 0])
                landed(homed.at[lay], r_home.at[lay, 1])

    for t in range(nl):
        own(t, wait, wait_send)
        p1(t, wait_send)
        zsend(t, False, wait, wait_send)
    for group in (scatter(), along_z(), forward_z(), gather(), to_sibling(0), to_sibling(1), to_sibling(2)):
        for cp in group:
            cp.wait_send()


def place_kernel(slots_ref, home13, homed, hot13, hotd, w13, wd, zero13, zerod, sem):
    n = lax.axis_index('stage') * 8 + lax.axis_index('expert')
    nlay = home13.shape[0]

    def home():
        yield pltpu.make_async_copy(home13, w13.at[:, 0], sem.at[0, 0])
        yield pltpu.make_async_copy(homed, wd.at[:, 0], sem.at[0, 1])

    for cp in home():
        cp.start()
    zero13[...] = jnp.zeros_like(zero13)
    zerod[...] = jnp.zeros_like(zerod)

    def fill(act):
        for h in range(2):
            used = slots_ref[n, h] >= 0

            @pl.when(used)
            def _():
                act(pltpu.make_async_copy(hot13, w13.at[:, 1 + h], sem.at[1 + h, 0]))
                act(pltpu.make_async_copy(hotd, wd.at[:, 1 + h], sem.at[1 + h, 1]))

            @pl.when(jnp.logical_not(used))
            def _():
                for lay in range(nlay):
                    act(pltpu.make_async_copy(zero13, w13.at[lay, 1 + h], sem.at[3 + h, 2 * lay]))
                    act(pltpu.make_async_copy(zerod, wd.at[lay, 1 + h], sem.at[3 + h, 2 * lay + 1]))

    fill(lambda cp: cp.start())
    fill(lambda cp: cp.wait())
    for cp in home():
        cp.wait()


def solution(mesh):
    flat = ('stage', 'expert')
    any_spec = pl.BlockSpec(memory_space=pl.ANY)
    smem = pl.BlockSpec(memory_space=pltpu.SMEM)
    vmem = pl.BlockSpec(memory_space=pltpu.VMEM)

    def body(gate, up, down, hot_units, slot_map):
        nl, _, dm, f4 = gate.shape
        ff = f4 // 4
        lay = nl * 4
        dma = pltpu.SemaphoreType.DMA
        shapes = [(lay, dm, 2 * ff), (lay, ff, dm)] * 2
        outs = pl.pallas_call(
            functools.partial(exchange_kernel, (nl, dm, ff)),
            out_shape=[pltpu.VMEM(s, BF16) for s in shapes],
            in_specs=[smem, any_spec, any_spec, any_spec],
            out_specs=[vmem] * 4,
            scratch_shapes=[
                pltpu.VMEM((4, nl, dm, ff), BF16), pltpu.VMEM((4, nl, dm, ff), BF16), pltpu.VMEM((4, nl, ff, dm), BF16),
                pltpu.VMEM((nl, dm, 2 * ff), BF16), pltpu.VMEM((nl, ff, dm), BF16),
                pltpu.VMEM((3, nl, dm, 2 * ff), BF16), pltpu.VMEM((3, nl, ff, dm), BF16),
                pltpu.VMEM((8, nl, dm // 8, 2 * ff), BF16), pltpu.VMEM((8, nl, ff // 8, dm), BF16),
                pltpu.VMEM((nl, dm // 8, 2 * ff), BF16), pltpu.VMEM((nl, ff // 8, dm), BF16),
                dma((2, nl, 3)), dma((2, 2, nl, 3)), dma((3, nl, 2)), dma((8, 2)), dma((3, 2)), dma((7, 2)),
                dma((3, nl, 2)), dma((lay, 2)), dma((8, 2)), dma((4, 2)), dma((8, 2)),
                dma((nl, 3)), dma((nl, 2)), dma((4, 3)), dma((4,)),
            ],
            compiler_params=pltpu.CompilerParams(has_side_effects=True, vmem_limit_bytes=44 << 20),
            name='exchange',
        )(hot_units, gate, up, down)
        return pl.pallas_call(
            place_kernel,
            out_shape=[jax.ShapeDtypeStruct((lay, 3, dm, 2 * ff), BF16), jax.ShapeDtypeStruct((lay, 3, ff, dm), BF16)],
            in_specs=[smem] + [vmem] * 4,
            out_specs=[any_spec] * 2,
            scratch_shapes=[pltpu.VMEM((dm, 2 * ff), BF16), pltpu.VMEM((ff, dm), BF16), dma((5, 2 * lay))],
            compiler_params=pltpu.CompilerParams(vmem_limit_bytes=20 << 20),
            name='place',
        )(slot_map, *outs)

    specs = P('stage', 'expert')
    return jax.shard_map(body, mesh=mesh, in_specs=(specs, specs, specs, P(), P()),
                         out_specs=(P(None, flat), P(None, flat)), check_vma=False)
```

```python
import functools

import jax
import jax.numpy as jnp
from jax import lax
from jax.experimental import pallas as pl
from jax.experimental.pallas import tpu as pltpu
from jax.sharding import PartitionSpec as P

MESH = pl.DeviceIdType.MESH
ORDER = (
    'load', 'own0', 'in00', 'in01', 'build', 'in02', 'in03', 'pair', 'z00', 'merge', 'scatter', 'in10', 'in11',
    'in12', 'in13', 'in20', 'in21', 'in22', 'in23', 'z01', 'z02', 'z03', 'select', 'alongz', 'own1', 'z10', 'z11',
    'fwd', 'z12', 'z13', 'own2', 'gather', 'z20', 'z21', 'z22', 'z23', 'sib',
)
CUTS = (((0, 1), (1, 1), (2, 2), (4, 4)), ((0, 2), (2, 2), (4, 2), (6, 2)), ((0, 2), (2, 2), (4, 2), (6, 2)))
BF16 = jnp.bfloat16


def exchange_kernel(dims, hot_ref, gate, up, down, home13, homed, hot13, hotd,
                    part_g, part_u, part_d, pair13, paird, give13, gived, mine13, mined, rel13, reld,
                    got13, gotd, sel13, seld,
                    s_own, s_p1, s_z, s_pair, s_hs, s_hz, s_hp,
                    r_rel, r_home, r_pair, r_hs, r_hz, r_hp, l_own, l_rel, l_part, l_hot):
    nl, dm, ff = dims
    z = lax.axis_index('stage')
    j = lax.axis_index('expert')
    y, x, c = j // 4, (j // 2) % 2, j % 2
    zt = j // 2
    r8 = dm // 8
    d8 = ff // 8

    def dev(zz, yy, xx, cc):
        return (zz, 4 * yy + 2 * xx + cc)

    def rdma(src, dst, ss, rs, to):
        return pltpu.make_async_remote_copy(src_ref=src, dst_ref=dst, send_sem=ss, recv_sem=rs,
                                            device_id=to, device_id_type=MESH)

    def landed(ref, sem):
        rdma(ref, ref, sem, sem, (z, j)).wait_recv()

    def cols(k):
        return pl.ds(pl.multiple_of(k * ff, ff), ff)

    def pieces(t, k, dst13, dstd):
        return ((gate.at[t, 0, :, cols(k)], dst13.at[:, pl.ds(0, ff)]),
                (up.at[t, 0, :, cols(k)], dst13.at[:, pl.ds(ff, ff)]),
                (down.at[t, 0, cols(k), :], dstd))

    def own(t, do_local, do_remote):
        lay = nl * z + t
        for kc in range(2):
            k = 2 * x + kc
            todo = pieces(t, k, home13.at[lay], homed.at[lay])
            stays = jnp.logical_and(z == zt, c == kc)

            @pl.when(jnp.logical_and(c == y, stays))
            def _():
                for a, (src, dst) in enumerate(todo):
                    do_local(pltpu.make_async_copy(src, dst, l_own.at[t, a]))

            @pl.when(jnp.logical_and(c == y, jnp.logical_not(stays)))
            def _():
                for a, (src, dst) in enumerate(todo):
                    do_remote(rdma(src, dst, s_own.at[kc, t, a], r_home.at[lay, a // 2], dev(zt, y, x, kc)))

    def rows(t, p):
        e0, n = CUTS[t][p]
        return pl.ds(e0 * r8, n * r8), pl.ds(e0 * d8, n * d8)

    def p1(t, p, do):
        r13, rd = rows(t, p)

        def to(dx, m, slot):
            xx = (x + dx) % 2
            for kc in range(2):
                k = 2 * xx + kc
                todo = ((gate.at[t, 0, r13, cols(k)], rel13.at[m, t, r13, pl.ds(0, ff)]),
                        (up.at[t, 0, r13, cols(k)], rel13.at[m, t, r13, pl.ds(ff, ff)]),
                        (down.at[t, 0, pl.ds(pl.multiple_of(k * ff + rd.start, d8), rd.size), :], reld.at[m, t, rd]))
                for a, (src, dst) in enumerate(todo):
                    do(rdma(src, dst, s_p1.at[slot, kc, t, p, a], r_rel.at[m, t, p, a // 2], dev(z, c, xx, kc)))

        @pl.when(c == y)
        def _():
            to(1, 0, 0)

        @pl.when(c != y)
        def _():
            to(0, 1, 0)
            to(1, 2, 1)

    relays = ((2 * y + 1 - x), (2 * (1 - y) + x), (2 * (1 - y) + 1 - x))

    def zsend(t, p, ms, wait, do_local, do_remote):
        lay = nl * z + t
        r13, rd = rows(t, p)
        for m in ms:
            zm = relays[m]
            src = (rel13.at[m, t, r13], reld.at[m, t, rd])
            dst = (home13.at[lay, r13], homed.at[lay, rd])
            if wait:
                for a in range(2):
                    landed(src[a], r_rel.at[m, t, p, a])

            @pl.when(zm == z)
            def _():
                for a in range(2):
                    do_local(pltpu.make_async_copy(src[a], dst[a], l_rel.at[t, p, a]))

            @pl.when(zm != z)
            def _():
                for a in range(2):
                    do_remote(rdma(src[a], dst[a], s_z.at[m, t, p, a], r_home.at[lay, a], (zm, j)))

    start = lambda cp: cp.start()
    wait_send = lambda cp: cp.wait_send()
    wait = lambda cp: cp.wait()

    def part_loads():
        for k in range(4):
            yield pltpu.make_async_copy(gate.at[:, 0, :, pl.ds(k * ff, ff)], part_g.at[k], l_part.at[k, 0])
            yield pltpu.make_async_copy(up.at[:, 0, :, pl.ds(k * ff, ff)], part_u.at[k], l_part.at[k, 1])
            yield pltpu.make_async_copy(down.at[:, 0, pl.ds(k * ff, ff), :], part_d.at[k], l_part.at[k, 2])

    def rows13(q):
        return pl.ds(pl.multiple_of(q * r8, r8), r8)

    def rowsd(q):
        return pl.ds(pl.multiple_of(q * d8, d8), d8)

    chip = j // 2

    def pair():
        to = dev(z, y, x, 1 - c)
        yield rdma(give13, pair13.at[c], s_pair.at[0], r_pair.at[0], to)
        yield rdma(gived, paird.at[c], s_pair.at[1], r_pair.at[1], to)

    def scatter_local():
        yield pltpu.make_async_copy(mine13.at[chip], got13.at[chip], l_hot.at[0])
        yield pltpu.make_async_copy(mined.at[chip], gotd.at[chip], l_hot.at[1])

    same_core = ((y, 1 - x), (1 - y, x), (1 - y, 1 - x))

    def scatter():
        for i, (yy, xx) in enumerate(same_core):
            q = 2 * yy + xx
            yield rdma(mine13.at[q], got13.at[chip], s_hs.at[i, 0], r_hs.at[chip, 0], dev(z, yy, xx, c))
            yield rdma(mined.at[q], gotd.at[chip], s_hs.at[i, 1], r_hs.at[chip, 1], dev(z, yy, xx, c))

    def hot_piece(zz, q):
        ls = pl.ds(nl * zz, nl)
        return hot13.at[ls, rows13(q), :], hotd.at[ls, rowsd(q), :]

    def hot_rows(q):
        return hot13.at[:, rows13(q), :], hotd.at[:, rowsd(q), :]

    z1 = z + 1 - 2 * (z % 2)
    zc = 3 - z
    zf = 3 - z1

    def sel_local():
        p13, pd = hot_piece(z, j)
        yield pltpu.make_async_copy(sel13, p13, l_hot.at[2])
        yield pltpu.make_async_copy(seld, pd, l_hot.at[3])

    def along_z():
        p13, pd = hot_piece(z, j)
        for i, to in enumerate((zc, z1)):
            yield rdma(sel13, p13, s_hz.at[i, 0], r_hz.at[z, 0], (to, j))
            yield rdma(seld, pd, s_hz.at[i, 1], r_hz.at[z, 1], (to, j))

    def forward_z():
        p13, pd = hot_piece(zc, j)
        yield rdma(p13, p13, s_hz.at[2, 0], r_hz.at[zc, 0], (z1, j))
        yield rdma(pd, pd, s_hz.at[2, 1], r_hz.at[zc, 1], (z1, j))

    def hot_z_landed(zz):
        for a, ref in enumerate(hot_piece(zz, j)):
            landed(ref, r_hz.at[zz, a])

    def gather():
        p13, pd = hot_rows(j)
        for i, (yy, xx) in enumerate(same_core):
            yield rdma(p13, p13, s_hp.at[i, 0], r_hp.at[j, 0], dev(z, yy, xx, c))
            yield rdma(pd, pd, s_hp.at[i, 1], r_hp.at[j, 1], dev(z, yy, xx, c))
        yield rdma(p13, p13, s_hp.at[3, 0], r_hp.at[j, 0], dev(z, y, x, 1 - c))
        yield rdma(pd, pd, s_hp.at[3, 1], r_hp.at[j, 1], dev(z, y, x, 1 - c))

    def hot_rows_landed(q):
        for a, ref in enumerate(hot_rows(q)):
            landed(ref, r_hp.at[q, a])

    def to_sibling(i):
        yy, xx = same_core[i]
        q = 4 * yy + 2 * xx + c
        p13, pd = hot_rows(q)
        yield rdma(p13, p13, s_hp.at[4 + i, 0], r_hp.at[q, 0], dev(z, y, x, 1 - c))
        yield rdma(pd, pd, s_hp.at[4 + i, 1], r_hp.at[q, 1], dev(z, y, x, 1 - c))

    def build_all():
        for cp in part_loads():
            cp.wait()
        kh = lax.rem(hot_ref[0], 4)

        def build(i, carry):
            t, b = i // 4, i % 4
            for par, to13, tod in ((1 - c, give13, gived), (c, pair13.at[c], paird.at[c])):
                rr = pl.ds(pl.multiple_of((2 * b + par) * r8, r8), r8)
                rd = pl.ds(pl.multiple_of((2 * b + par) * d8, d8), d8)
                to13[b, t, :, 0:ff] = part_g[kh, t, rr, :]
                to13[b, t, :, ff:2 * ff] = part_u[kh, t, rr, :]
                tod[b, t] = part_d[kh, t, rd, :]
            return carry

        lax.fori_loop(0, nl * 4, build, 0)

    def merge():
        landed(pair13.at[1 - c], r_pair.at[0])
        landed(paird.at[1 - c], r_pair.at[1])
        core = lax.rem(hot_ref[0] // 4, 2)

        def pick(i, carry):
            b, t = i // nl, i % nl
            mine13[b, t] = pair13[core, b, t]
            mined[b, t] = paird[core, b, t]
            return carry

        lax.fori_loop(0, nl * 4, pick, 0)

    def run(group):
        for cp in group:
            cp.start()

    def select():
        for cp in scatter_local():
            cp.wait()
        for yy, xx in same_core:
            q = 2 * yy + xx
            landed(got13.at[q], r_hs.at[q, 0])
            landed(gotd.at[q], r_hs.at[q, 1])
        owner = lax.div(hot_ref[0], 8)
        sel13[...] = got13[owner]
        seld[...] = gotd[owner]

    def sct():
        run(scatter_local())
        run(scatter())

    def alongz():
        run(along_z())
        run(sel_local())

    def fwd():
        hot_z_landed(zc)
        run(forward_z())

    def gat():
        for cp in sel_local():
            cp.wait()
        hot_z_landed(z1)
        hot_z_landed(zf)
        run(gather())

    def sib():
        for i in range(3):
            yy, xx = same_core[i]
            hot_rows_landed(4 * yy + 2 * xx + c)
            run(to_sibling(i))

    steps = dict(load=lambda: run(part_loads()), build=build_all, pair=lambda: run(pair()), merge=merge, scatter=sct,
                 select=select, alongz=alongz, fwd=fwd, gather=gat, sib=sib)
    for t in range(nl):
        steps[f'own{t}'] = functools.partial(own, t, start, start)
        for p in range(len(CUTS[t])):
            steps[f'in{t}{p}'] = functools.partial(p1, t, p, start)
            steps[f'z{t}{p}'] = functools.partial(zsend, t, p, range(3), True, start, start)
            for m in range(3):
                steps[f'z{t}{p}{m}'] = functools.partial(zsend, t, p, (m,), True, start, start)
    for step in ORDER:
        steps[step]()

    for yy in range(2):
        for xx in range(2):
            hot_rows_landed(4 * yy + 2 * xx + 1 - c)
    for zz in range(4):
        for t in range(nl):
            lay = nl * zz + t
            away = z != zz
            sib = jnp.logical_and(z == zt, c != y)

            @pl.when(jnp.logical_or(away, sib))
            def _():
                landed(home13.at[lay], r_home.at[lay, 0])
                landed(homed.at[lay], r_home.at[lay, 1])

    for t in range(nl):
        own(t, wait, wait_send)
        for p in range(len(CUTS[t])):
            p1(t, p, wait_send)
            zsend(t, p, range(3), False, wait, wait_send)
    for group in (pair(), scatter(), along_z(), forward_z(), gather(), to_sibling(0), to_sibling(1), to_sibling(2)):
        for cp in group:
            cp.wait_send()


def place_kernel(slots_ref, home13, homed, hot13, hotd, w13, wd, zero13, zerod, sem):
    n = lax.axis_index('stage') * 8 + lax.axis_index('expert')
    nlay = home13.shape[0]

    def home():
        yield pltpu.make_async_copy(home13, w13.at[:, 0], sem.at[0, 0])
        yield pltpu.make_async_copy(homed, wd.at[:, 0], sem.at[0, 1])

    for cp in home():
        cp.start()
    zero13[...] = jnp.zeros_like(zero13)
    zerod[...] = jnp.zeros_like(zerod)

    def fill(act):
        for h in range(2):
            used = slots_ref[n, h] >= 0

            @pl.when(used)
            def _():
                act(pltpu.make_async_copy(hot13, w13.at[:, 1 + h], sem.at[1 + h, 0]))
                act(pltpu.make_async_copy(hotd, wd.at[:, 1 + h], sem.at[1 + h, 1]))

            @pl.when(jnp.logical_not(used))
            def _():
                for lay in range(nlay):
                    act(pltpu.make_async_copy(zero13, w13.at[lay, 1 + h], sem.at[3 + h, 2 * lay]))
                    act(pltpu.make_async_copy(zerod, wd.at[lay, 1 + h], sem.at[3 + h, 2 * lay + 1]))

    fill(lambda cp: cp.start())
    fill(lambda cp: cp.wait())
    for cp in home():
        cp.wait()


def solution(mesh):
    flat = ('stage', 'expert')
    any_spec = pl.BlockSpec(memory_space=pl.ANY)
    smem = pl.BlockSpec(memory_space=pltpu.SMEM)
    vmem = pl.BlockSpec(memory_space=pltpu.VMEM)

    def body(gate, up, down, hot_units, slot_map):
        nl, _, dm, f4 = gate.shape
        ff = f4 // 4
        lay = nl * 4
        r8, d8 = dm // 8, ff // 8
        cut = max(map(len, CUTS))
        dma = pltpu.SemaphoreType.DMA
        shapes = [(lay, dm, 2 * ff), (lay, ff, dm)] * 2
        outs = pl.pallas_call(
            functools.partial(exchange_kernel, (nl, dm, ff)),
            out_shape=[pltpu.VMEM(s, BF16) for s in shapes],
            in_specs=[smem, any_spec, any_spec, any_spec],
            out_specs=[vmem] * 4,
            scratch_shapes=[
                pltpu.VMEM((4, nl, dm, ff), BF16), pltpu.VMEM((4, nl, dm, ff), BF16), pltpu.VMEM((4, nl, ff, dm), BF16),
                pltpu.VMEM((2, 4, nl, r8, 2 * ff), BF16), pltpu.VMEM((2, 4, nl, d8, dm), BF16),
                pltpu.VMEM((4, nl, r8, 2 * ff), BF16), pltpu.VMEM((4, nl, d8, dm), BF16),
                pltpu.VMEM((4, nl, r8, 2 * ff), BF16), pltpu.VMEM((4, nl, d8, dm), BF16),
                pltpu.VMEM((3, nl, dm, 2 * ff), BF16), pltpu.VMEM((3, nl, ff, dm), BF16),
                pltpu.VMEM((4, nl, r8, 2 * ff), BF16), pltpu.VMEM((4, nl, d8, dm), BF16),
                pltpu.VMEM((nl, r8, 2 * ff), BF16), pltpu.VMEM((nl, d8, dm), BF16),
                dma((2, nl, 3)), dma((2, 2, nl, cut, 3)), dma((3, nl, cut, 2)), dma((2,)), dma((3, 2)), dma((3, 2)), dma((7, 2)),
                dma((3, nl, cut, 2)), dma((lay, 2)), dma((2,)), dma((4, 2)), dma((4, 2)), dma((8, 2)),
                dma((nl, 3)), dma((nl, cut, 2)), dma((4, 3)), dma((4,)),
            ],
            compiler_params=pltpu.CompilerParams(has_side_effects=True, vmem_limit_bytes=44 << 20),
            name='exchange',
        )(hot_units, gate, up, down)
        return pl.pallas_call(
            place_kernel,
            out_shape=[jax.ShapeDtypeStruct((lay, 3, dm, 2 * ff), BF16), jax.ShapeDtypeStruct((lay, 3, ff, dm), BF16)],
            in_specs=[smem] + [vmem] * 4,
            out_specs=[any_spec] * 2,
            scratch_shapes=[pltpu.VMEM((dm, 2 * ff), BF16), pltpu.VMEM((ff, dm), BF16), dma((5, 2 * lay))],
            compiler_params=pltpu.CompilerParams(vmem_limit_bytes=20 << 20),
            name='place',
        )(slot_map, *outs)

    specs = P('stage', 'expert')
    return jax.shard_map(body, mesh=mesh, in_specs=(specs, specs, specs, P(), P()),
                         out_specs=(P(None, flat), P(None, flat)), check_vma=False)
```

```python
import functools

import jax
import jax.numpy as jnp
from jax import lax
from jax.experimental import pallas as pl
from jax.experimental.pallas import tpu as pltpu
from jax.sharding import PartitionSpec as P

MESH = pl.DeviceIdType.MESH
ORDER = (
    'in00', 'own0', 'in01', 'load', 'zf0', 'in02', 'zf1', 'in03', 'build', 'pair', 'merge', 'scatter', 'in10',
    'in11', 'in20', 'in21', 'z02', 'z03', 'select', 'alongz', 'z10', 'z11', 'fwd', 'z20', 'gather', 'z21', 'sib',
)
CUTS = (((0, 1), (1, 1), (2, 2), (4, 4)), ((0, 4), (4, 4)), ((0, 4), (4, 4)))
BF16 = jnp.bfloat16


def exchange_kernel(dims, hot_ref, gate, up, down, home13, homed, hot13, hotd,
                    part_g, part_u, part_d, pair13, paird, give13, gived, mine13, mined, rel13, reld,
                    got13, gotd, sel13, seld,
                    s_own, s_p1, s_z, s_pair, s_hs, s_hz, s_hp,
                    r_rel, r_home, r_pair, r_hs, r_hz, r_hp, l_own, l_rel, l_part, l_hot):
    nl, dm, ff = dims
    z = lax.axis_index('stage')
    j = lax.axis_index('expert')
    y, x, c = j // 4, (j // 2) % 2, j % 2
    zt = j // 2
    r8 = dm // 8
    d8 = ff // 8

    def dev(zz, yy, xx, cc):
        return (zz, 4 * yy + 2 * xx + cc)

    def rdma(src, dst, ss, rs, to):
        return pltpu.make_async_remote_copy(src_ref=src, dst_ref=dst, send_sem=ss, recv_sem=rs,
                                            device_id=to, device_id_type=MESH)

    def landed(ref, sem):
        rdma(ref, ref, sem, sem, (z, j)).wait_recv()

    def cols(k):
        return pl.ds(pl.multiple_of(k * ff, ff), ff)

    def pieces(t, k, dst13, dstd):
        return ((gate.at[t, 0, :, cols(k)], dst13.at[:, pl.ds(0, ff)]),
                (up.at[t, 0, :, cols(k)], dst13.at[:, pl.ds(ff, ff)]),
                (down.at[t, 0, cols(k), :], dstd))

    start = lambda cp: cp.start()
    wait_send = lambda cp: cp.wait_send()
    wait = lambda cp: cp.wait()

    def own(t, do_local, do_remote):
        lay = nl * z + t
        for kc in range(2):
            k = 2 * x + kc
            todo = pieces(t, k, home13.at[lay], homed.at[lay])
            stays = jnp.logical_and(z == zt, c == kc)

            @pl.when(jnp.logical_and(c == y, stays))
            def _():
                for a, (src, dst) in enumerate(todo):
                    do_local(pltpu.make_async_copy(src, dst, l_own.at[t, a]))

            @pl.when(jnp.logical_and(c == y, jnp.logical_not(stays)))
            def _():
                for a, (src, dst) in enumerate(todo):
                    do_remote(rdma(src, dst, s_own.at[kc, t, a], r_home.at[lay, a // 2], dev(zt, y, x, kc)))

    def rows(t, p):
        e0, n = CUTS[t][p]
        return pl.ds(e0 * r8, n * r8), pl.ds(e0 * d8, n * d8)

    def p1(t, p, do):
        r13, rd = rows(t, p)

        def to(dx, m, slot):
            xx = (x + dx) % 2
            for kc in range(2):
                k = 2 * xx + kc
                todo = ((gate.at[t, 0, r13, cols(k)], rel13.at[m, t, r13, pl.ds(0, ff)]),
                        (up.at[t, 0, r13, cols(k)], rel13.at[m, t, r13, pl.ds(ff, ff)]),
                        (down.at[t, 0, pl.ds(pl.multiple_of(k * ff + rd.start, d8), rd.size), :], reld.at[m, t, rd]))
                for a, (src, dst) in enumerate(todo):
                    do(rdma(src, dst, s_p1.at[slot, kc, t, p, a], r_rel.at[m, t, p, a // 2], dev(z, c, xx, kc)))

        @pl.when(c == y)
        def _():
            to(1, 0, 0)

        @pl.when(c != y)
        def _():
            to(0, 1, 0)
            to(1, 2, 1)

    first = 1 - abs(y - z // 2)

    def soonest(i):
        m = (i + first) % 3
        return m, 2 * ((y + (m + 1) // 2) % 2) + (x + 1 - m * (2 - m)) % 2

    def relay(i):
        up = 1 - z // 2
        near = z * up + (3 - z) * (1 - up)
        zd = (3, 2, 1 - near, near)[i]
        zd = zd * up + (3 - zd) * (1 - up)
        dx = (zd % 2 + x) % 2
        dy = (zd // 2 + y) % 2
        return jnp.logical_or(dx > 0, dy > 0), dy * (1 + dx), zd

    def zfirst(p):
        r13, rd = rows(0, p)
        for i in range(3):
            m, zd = soonest(i)
            src = (rel13.at[m, 0, r13], reld.at[m, 0, rd])
            dst = (home13.at[nl * z, r13], homed.at[nl * z, rd])
            for a in range(2):
                landed(src[a], r_rel.at[m, 0, p, a])

            @pl.when(zd == z)
            def _():
                for a in range(2):
                    pltpu.make_async_copy(src[a], dst[a], l_rel.at[0, p, a]).start()

            for k in range(3):
                _, _, zk = relay(k)

                @pl.when(zd == zk)
                def _():
                    for a in range(2):
                        rdma(src[a], dst[a], s_z.at[k, 0, p, a], r_home.at[nl * z, a], (zk, j)).start()

    def zsend(t, p, wait, do_local, do_remote):
        lay = nl * z + t
        r13, rd = rows(t, p)
        for i in range(4):
            held, m, zd = relay(i)
            src = (rel13.at[m, t, r13], reld.at[m, t, rd])
            dst = (home13.at[lay, r13], homed.at[lay, rd])

            @pl.when(held)
            def _():
                for a in range(2):
                    if wait:
                        landed(src[a], r_rel.at[m, t, p, a])
                    if i == 3:
                        do_local(pltpu.make_async_copy(src[a], dst[a], l_rel.at[t, p, a]))
                    else:
                        do_remote(rdma(src[a], dst[a], s_z.at[i, t, p, a], r_home.at[lay, a], (zd, j)))

            if wait and t > 0 and p == 0:
                @pl.when(jnp.logical_not(held))
                def _():
                    own(t, start, start)


    def part_loads():
        for k in range(4):
            yield pltpu.make_async_copy(gate.at[:, 0, :, pl.ds(k * ff, ff)], part_g.at[k], l_part.at[k, 0])
            yield pltpu.make_async_copy(up.at[:, 0, :, pl.ds(k * ff, ff)], part_u.at[k], l_part.at[k, 1])
            yield pltpu.make_async_copy(down.at[:, 0, pl.ds(k * ff, ff), :], part_d.at[k], l_part.at[k, 2])

    def rows13(q):
        return pl.ds(pl.multiple_of(q * r8, r8), r8)

    def rowsd(q):
        return pl.ds(pl.multiple_of(q * d8, d8), d8)

    chip = j // 2

    def pair():
        to = dev(z, y, x, 1 - c)
        yield rdma(give13, pair13.at[c], s_pair.at[0], r_pair.at[0], to)
        yield rdma(gived, paird.at[c], s_pair.at[1], r_pair.at[1], to)

    def scatter_local():
        yield pltpu.make_async_copy(mine13.at[chip], got13.at[chip], l_hot.at[0])
        yield pltpu.make_async_copy(mined.at[chip], gotd.at[chip], l_hot.at[1])

    same_core = ((y, 1 - x), (1 - y, x), (1 - y, 1 - x))

    def scatter():
        for i, (yy, xx) in enumerate(same_core):
            q = 2 * yy + xx
            yield rdma(mine13.at[q], got13.at[chip], s_hs.at[i, 0], r_hs.at[chip, 0], dev(z, yy, xx, c))
            yield rdma(mined.at[q], gotd.at[chip], s_hs.at[i, 1], r_hs.at[chip, 1], dev(z, yy, xx, c))

    def hot_piece(zz, q):
        ls = pl.ds(nl * zz, nl)
        return hot13.at[ls, rows13(q), :], hotd.at[ls, rowsd(q), :]

    def hot_rows(q):
        return hot13.at[:, rows13(q), :], hotd.at[:, rowsd(q), :]

    z1 = z + 1 - 2 * (z % 2)
    zc = 3 - z
    zf = 3 - z1

    def sel_local():
        p13, pd = hot_piece(z, j)
        yield pltpu.make_async_copy(sel13, p13, l_hot.at[2])
        yield pltpu.make_async_copy(seld, pd, l_hot.at[3])

    def along_z():
        p13, pd = hot_piece(z, j)
        for i, to in enumerate((zc, z1)):
            yield rdma(sel13, p13, s_hz.at[i, 0], r_hz.at[z, 0], (to, j))
            yield rdma(seld, pd, s_hz.at[i, 1], r_hz.at[z, 1], (to, j))

    def forward_z():
        p13, pd = hot_piece(zc, j)
        yield rdma(p13, p13, s_hz.at[2, 0], r_hz.at[zc, 0], (z1, j))
        yield rdma(pd, pd, s_hz.at[2, 1], r_hz.at[zc, 1], (z1, j))

    def hot_z_landed(zz):
        for a, ref in enumerate(hot_piece(zz, j)):
            landed(ref, r_hz.at[zz, a])

    def gather():
        p13, pd = hot_rows(j)
        for i, (yy, xx) in enumerate(same_core):
            yield rdma(p13, p13, s_hp.at[i, 0], r_hp.at[j, 0], dev(z, yy, xx, c))
            yield rdma(pd, pd, s_hp.at[i, 1], r_hp.at[j, 1], dev(z, yy, xx, c))
        yield rdma(p13, p13, s_hp.at[3, 0], r_hp.at[j, 0], dev(z, y, x, 1 - c))
        yield rdma(pd, pd, s_hp.at[3, 1], r_hp.at[j, 1], dev(z, y, x, 1 - c))

    def hot_rows_landed(q):
        for a, ref in enumerate(hot_rows(q)):
            landed(ref, r_hp.at[q, a])

    def to_sibling(i):
        yy, xx = same_core[i]
        q = 4 * yy + 2 * xx + c
        p13, pd = hot_rows(q)
        yield rdma(p13, p13, s_hp.at[4 + i, 0], r_hp.at[q, 0], dev(z, y, x, 1 - c))
        yield rdma(pd, pd, s_hp.at[4 + i, 1], r_hp.at[q, 1], dev(z, y, x, 1 - c))

    def build_all():
        for cp in part_loads():
            cp.wait()
        kh = lax.rem(hot_ref[0], 4)

        def build(i, carry):
            t, b = i // 4, i % 4
            for par, to13, tod in ((1 - c, give13, gived), (c, pair13.at[c], paird.at[c])):
                rr = pl.ds(pl.multiple_of((2 * b + par) * r8, r8), r8)
                rd = pl.ds(pl.multiple_of((2 * b + par) * d8, d8), d8)
                to13[b, t, :, 0:ff] = part_g[kh, t, rr, :]
                to13[b, t, :, ff:2 * ff] = part_u[kh, t, rr, :]
                tod[b, t] = part_d[kh, t, rd, :]
            return carry

        lax.fori_loop(0, nl * 4, build, 0)

    def merge():
        landed(pair13.at[1 - c], r_pair.at[0])
        landed(paird.at[1 - c], r_pair.at[1])
        core = lax.rem(hot_ref[0] // 4, 2)

        def pick(i, carry):
            b, t = i // nl, i % nl
            mine13[b, t] = pair13[core, b, t]
            mined[b, t] = paird[core, b, t]
            return carry

        lax.fori_loop(0, nl * 4, pick, 0)

    def run(group):
        for cp in group:
            cp.start()

    def select():
        for cp in scatter_local():
            cp.wait()
        for yy, xx in same_core:
            q = 2 * yy + xx
            landed(got13.at[q], r_hs.at[q, 0])
            landed(gotd.at[q], r_hs.at[q, 1])
        owner = lax.div(hot_ref[0], 8)
        sel13[...] = got13[owner]
        seld[...] = gotd[owner]

    def sct():
        run(scatter_local())
        run(scatter())

    def alongz():
        run(along_z())
        run(sel_local())

    def fwd():
        hot_z_landed(zc)
        run(forward_z())

    def gat():
        for cp in sel_local():
            cp.wait()
        hot_z_landed(z1)
        hot_z_landed(zf)
        run(gather())

    def sib():
        for i in range(3):
            yy, xx = same_core[i]
            hot_rows_landed(4 * yy + 2 * xx + c)
            run(to_sibling(i))

    steps = dict(load=lambda: run(part_loads()), build=build_all, pair=lambda: run(pair()), merge=merge, scatter=sct,
                 select=select, alongz=alongz, fwd=fwd, gather=gat, sib=sib)
    for p in range(len(CUTS[0])):
        steps[f'zf{p}'] = functools.partial(zfirst, p)
    for t in range(nl):
        steps[f'own{t}'] = functools.partial(own, t, start, start)
        for p in range(len(CUTS[t])):
            steps[f'in{t}{p}'] = functools.partial(p1, t, p, start)
            steps[f'z{t}{p}'] = functools.partial(zsend, t, p, True, start, start)
    for step in ORDER:
        steps[step]()

    for yy in range(2):
        for xx in range(2):
            hot_rows_landed(4 * yy + 2 * xx + 1 - c)
    for zz in range(4):
        for t in range(nl):
            lay = nl * zz + t
            away = z != zz
            sib = jnp.logical_and(z == zt, c != y)

            @pl.when(jnp.logical_or(away, sib))
            def _():
                landed(home13.at[lay], r_home.at[lay, 0])
                landed(homed.at[lay], r_home.at[lay, 1])

    for t in range(nl):
        own(t, wait, wait_send)
        for p in range(len(CUTS[t])):
            p1(t, p, wait_send)
            zsend(t, p, False, wait, wait_send)
    for group in (pair(), scatter(), along_z(), forward_z(), gather(), to_sibling(0), to_sibling(1), to_sibling(2)):
        for cp in group:
            cp.wait_send()


def place_kernel(slots_ref, home13, homed, hot13, hotd, w13, wd, zero13, zerod, sem):
    n = lax.axis_index('stage') * 8 + lax.axis_index('expert')
    nlay = home13.shape[0]
    step = nlay // 4

    def put(slot, src13, srcd, act):
        for i in range(0, nlay, step):
            ls = pl.ds(i, step)
            act(pltpu.make_async_copy(src13.at[ls], w13.at[ls, slot], sem.at[slot, i, 0]))
            act(pltpu.make_async_copy(srcd.at[ls], wd.at[ls, slot], sem.at[slot, i, 1]))

    start = lambda cp: cp.start()
    wait = lambda cp: cp.wait()
    put(0, home13, homed, start)
    used = [slots_ref[h, n] >= 0 for h in range(2)]
    empty = jnp.logical_not(jnp.logical_and(*used))

    for h in range(2):
        @pl.when(used[h])
        def _():
            put(1 + h, hot13, hotd, start)

    def zeros(h, act):
        for lay in range(nlay):
            act(pltpu.make_async_copy(zero13, w13.at[lay, 1 + h], sem.at[3 + h, lay, 0]))
            act(pltpu.make_async_copy(zerod, wd.at[lay, 1 + h], sem.at[3 + h, lay, 1]))

    @pl.when(empty)
    def _():
        zero13[...] = jnp.zeros_like(zero13)
        zerod[...] = jnp.zeros_like(zerod)
        for h in range(2):
            pl.when(jnp.logical_not(used[h]))(functools.partial(zeros, h, start))
        for h in range(2):
            pl.when(jnp.logical_not(used[h]))(functools.partial(zeros, h, wait))

    for h in range(2):
        @pl.when(used[h])
        def _():
            put(1 + h, hot13, hotd, wait)
    put(0, home13, homed, wait)


def solution(mesh):
    flat = ('stage', 'expert')
    any_spec = pl.BlockSpec(memory_space=pl.ANY)
    smem = pl.BlockSpec(memory_space=pltpu.SMEM)
    vmem = pl.BlockSpec(memory_space=pltpu.VMEM)

    def body(gate, up, down, hot_units, slot_map):
        nl, _, dm, f4 = gate.shape
        ff = f4 // 4
        lay = nl * 4
        r8, d8 = dm // 8, ff // 8
        cut = max(map(len, CUTS))
        dma = pltpu.SemaphoreType.DMA
        shapes = [(lay, dm, 2 * ff), (lay, ff, dm)] * 2
        outs = pl.pallas_call(
            functools.partial(exchange_kernel, (nl, dm, ff)),
            out_shape=[pltpu.VMEM(s, BF16) for s in shapes],
            in_specs=[smem, any_spec, any_spec, any_spec],
            out_specs=[vmem] * 4,
            scratch_shapes=[
                pltpu.VMEM((4, nl, dm, ff), BF16), pltpu.VMEM((4, nl, dm, ff), BF16), pltpu.VMEM((4, nl, ff, dm), BF16),
                pltpu.VMEM((2, 4, nl, r8, 2 * ff), BF16), pltpu.VMEM((2, 4, nl, d8, dm), BF16),
                pltpu.VMEM((4, nl, r8, 2 * ff), BF16), pltpu.VMEM((4, nl, d8, dm), BF16),
                pltpu.VMEM((4, nl, r8, 2 * ff), BF16), pltpu.VMEM((4, nl, d8, dm), BF16),
                pltpu.VMEM((3, nl, dm, 2 * ff), BF16), pltpu.VMEM((3, nl, ff, dm), BF16),
                pltpu.VMEM((4, nl, r8, 2 * ff), BF16), pltpu.VMEM((4, nl, d8, dm), BF16),
                pltpu.VMEM((nl, r8, 2 * ff), BF16), pltpu.VMEM((nl, d8, dm), BF16),
                dma((2, nl, 3)), dma((2, 2, nl, cut, 3)), dma((3, nl, cut, 2)), dma((2,)), dma((3, 2)), dma((3, 2)), dma((7, 2)),
                dma((3, nl, cut, 2)), dma((lay, 2)), dma((2,)), dma((4, 2)), dma((4, 2)), dma((8, 2)),
                dma((nl, 3)), dma((nl, cut, 2)), dma((4, 3)), dma((4,)),
            ],
            compiler_params=pltpu.CompilerParams(has_side_effects=True, vmem_limit_bytes=44 << 20),
            name='exchange',
        )(hot_units, gate, up, down)
        return pl.pallas_call(
            place_kernel,
            out_shape=[jax.ShapeDtypeStruct((lay, 3, dm, 2 * ff), BF16), jax.ShapeDtypeStruct((lay, 3, ff, dm), BF16)],
            in_specs=[smem] + [vmem] * 4,
            out_specs=[any_spec] * 2,
            scratch_shapes=[pltpu.VMEM((dm, 2 * ff), BF16), pltpu.VMEM((ff, dm), BF16), dma((5, lay, 2))],
            compiler_params=pltpu.CompilerParams(vmem_limit_bytes=20 << 20),
            name='place',
        )(slot_map.T, *outs)

    specs = P('stage', 'expert')
    return jax.shard_map(body, mesh=mesh, in_specs=(specs, specs, specs, P(), P()),
                         out_specs=(P(None, flat), P(None, flat)), check_vma=False)
```

```python
import functools

import jax
import jax.numpy as jnp
from jax import lax
from jax.experimental import pallas as pl
from jax.experimental.pallas import tpu as pltpu
from jax.sharding import PartitionSpec as P

MESH = pl.DeviceIdType.MESH
ORDER = (
    'in00', 'own0', 'in01', 'load', 'zf0', 'in02', 'zf1', 'in03', 'build', 'pair', 'merge', 'scatter', 'in10',
    'in20', 'in21', 'z02', 'z03', 'select', 'alongz', 'z10', 'fwd', 'gather', 'z20', 'z21', 'sib',
)
CUTS = (((0, 1), (1, 1), (2, 2), (4, 4)), ((0, 8),), ((0, 7), (7, 1)))
DIRECT = ((2, 1),)
BF16 = jnp.bfloat16


def exchange_kernel(dims, hot_ref, gate, up, down, home13, homed, hot13, hotd,
                    part_g, part_u, part_d, pair13, paird, give13, gived, mine13, mined, rel13, reld,
                    got13, gotd, sel13, seld,
                    s_own, s_p1, s_z, s_pair, s_hs, s_hz, s_hp,
                    r_rel, r_home, r_pair, r_hs, r_hz, r_hp, l_own, l_rel, l_part, l_hot):
    nl, dm, ff = dims
    z = lax.axis_index('stage')
    j = lax.axis_index('expert')
    y, x, c = j // 4, (j // 2) % 2, j % 2
    zt = j // 2
    r8 = dm // 8
    d8 = ff // 8

    first = 1 - abs(y - z // 2)

    def dev(zz, yy, xx, cc):
        return (zz, 4 * yy + 2 * xx + cc)

    def rdma(src, dst, ss, rs, to):
        return pltpu.make_async_remote_copy(src_ref=src, dst_ref=dst, send_sem=ss, recv_sem=rs,
                                            device_id=to, device_id_type=MESH)

    def landed(ref, sem):
        rdma(ref, ref, sem, sem, (z, j)).wait_recv()

    def cols(k):
        return pl.ds(pl.multiple_of(k * ff, ff), ff)

    def pieces(t, k, dst13, dstd):
        return ((gate.at[t, 0, :, cols(k)], dst13.at[:, pl.ds(0, ff)]),
                (up.at[t, 0, :, cols(k)], dst13.at[:, pl.ds(ff, ff)]),
                (down.at[t, 0, cols(k), :], dstd))

    start = lambda cp: cp.start()
    wait_send = lambda cp: cp.wait_send()
    wait = lambda cp: cp.wait()

    def own(t, do_local, do_remote):
        lay = nl * z + t
        for kc in range(2):
            k = 2 * x + kc
            todo = pieces(t, k, home13.at[lay], homed.at[lay])
            stays = jnp.logical_and(z == zt, c == kc)

            @pl.when(jnp.logical_and(c == y, stays))
            def _():
                for a, (src, dst) in enumerate(todo):
                    do_local(pltpu.make_async_copy(src, dst, l_own.at[t, a]))

            @pl.when(jnp.logical_and(c == y, jnp.logical_not(stays)))
            def _():
                for a, (src, dst) in enumerate(todo):
                    do_remote(rdma(src, dst, s_own.at[kc, t, a], r_home.at[lay, a // 2], dev(zt, y, x, kc)))

    def rows(t, p):
        e0, n = CUTS[t][p]
        return pl.ds(e0 * r8, n * r8), pl.ds(e0 * d8, n * d8)

    def p1(t, p, do):
        r13, rd = rows(t, p)

        def to(dx, m, slot, direct=False, cores=(0, 1)):
            xx = (x + dx) % 2
            lay = nl * z + t
            dst13, dstd = (home13.at[lay], homed.at[lay]) if direct else (rel13.at[m, t], reld.at[m, t])
            for kc in cores:
                k = 2 * xx + kc
                todo = ((gate.at[t, 0, r13, cols(k)], dst13.at[r13, pl.ds(0, ff)]),
                        (up.at[t, 0, r13, cols(k)], dst13.at[r13, pl.ds(ff, ff)]),
                        (down.at[t, 0, pl.ds(pl.multiple_of(k * ff + rd.start, d8), rd.size), :], dstd.at[rd]))
                for a, (src, dst) in enumerate(todo):
                    recv = r_home.at[lay, a // 2] if direct else r_rel.at[m, t, p, a // 2]
                    do(rdma(src, dst, s_p1.at[slot, kc, t, p, a], recv, dev(zt if direct else z, c, xx, kc)))

        @pl.when(c == y)
        def _():
            to(1, 0, 0)

        if (t, p) in DIRECT:
            @pl.when(jnp.logical_and(c != y, first == 1))
            def _():
                to(0, 1, 0)

            @pl.when(jnp.logical_and(c != y, first == 0))
            def _():
                to(0, 1, 0, direct=True, cores=(0,))
                to(0, 1, 0, cores=(1,))
        else:
            @pl.when(c != y)
            def _():
                to(0, 1, 0)

        @pl.when(c != y)
        def _():
            to(1, 2, 1)

    def soonest(i):
        m = (i + first) % 3
        return m, 2 * ((y + (m + 1) // 2) % 2) + (x + 1 - m * (2 - m)) % 2

    def relay(i):
        up = 1 - z // 2
        near = z * up + (3 - z) * (1 - up)
        zd = (3, 2, 1 - near, near)[i]
        zd = zd * up + (3 - zd) * (1 - up)
        dx = (zd % 2 + x) % 2
        dy = (zd // 2 + y) % 2
        return jnp.logical_or(dx > 0, dy > 0), dy * (1 + dx), zd

    def zfirst(p):
        r13, rd = rows(0, p)
        for i in range(3):
            m, zd = soonest(i)
            src = (rel13.at[m, 0, r13], reld.at[m, 0, rd])
            dst = (home13.at[nl * z, r13], homed.at[nl * z, rd])
            for a in range(2):
                landed(src[a], r_rel.at[m, 0, p, a])

            @pl.when(zd == z)
            def _():
                for a in range(2):
                    pltpu.make_async_copy(src[a], dst[a], l_rel.at[0, p, a]).start()

            for k in range(3):
                _, _, zk = relay(k)

                @pl.when(zd == zk)
                def _():
                    for a in range(2):
                        rdma(src[a], dst[a], s_z.at[k, 0, p, a], r_home.at[nl * z, a], (zk, j)).start()

    def zsend(t, p, wait, do_local, do_remote):
        lay = nl * z + t
        r13, rd = rows(t, p)
        for i in range(4):
            held, m, zd = relay(i)
            own_here = jnp.logical_not(held)
            if (t, p) in DIRECT:
                held = jnp.logical_and(held, jnp.logical_or(m != 1, jnp.logical_or(first == 0, c == 1)))
            src = (rel13.at[m, t, r13], reld.at[m, t, rd])
            dst = (home13.at[lay, r13], homed.at[lay, rd])

            @pl.when(held)
            def _():
                for a in range(2):
                    if wait:
                        landed(src[a], r_rel.at[m, t, p, a])
                    if i == 3:
                        do_local(pltpu.make_async_copy(src[a], dst[a], l_rel.at[t, p, a]))
                    else:
                        do_remote(rdma(src[a], dst[a], s_z.at[i, t, p, a], r_home.at[lay, a], (zd, j)))

            if wait and t > 0 and p == 0:
                @pl.when(own_here)
                def _():
                    own(t, start, start)


    def part_loads():
        for k in range(4):
            yield pltpu.make_async_copy(gate.at[:, 0, :, pl.ds(k * ff, ff)], part_g.at[k], l_part.at[k, 0])
            yield pltpu.make_async_copy(up.at[:, 0, :, pl.ds(k * ff, ff)], part_u.at[k], l_part.at[k, 1])
            yield pltpu.make_async_copy(down.at[:, 0, pl.ds(k * ff, ff), :], part_d.at[k], l_part.at[k, 2])

    def rows13(q):
        return pl.ds(pl.multiple_of(q * r8, r8), r8)

    def rowsd(q):
        return pl.ds(pl.multiple_of(q * d8, d8), d8)

    chip = j // 2

    def pair():
        to = dev(z, y, x, 1 - c)
        yield rdma(give13, pair13.at[c], s_pair.at[0], r_pair.at[0], to)
        yield rdma(gived, paird.at[c], s_pair.at[1], r_pair.at[1], to)

    def scatter_local():
        yield pltpu.make_async_copy(mine13.at[chip], got13.at[chip], l_hot.at[0])
        yield pltpu.make_async_copy(mined.at[chip], gotd.at[chip], l_hot.at[1])

    same_core = ((y, 1 - x), (1 - y, x), (1 - y, 1 - x))

    def scatter():
        for i, (yy, xx) in enumerate(same_core):
            q = 2 * yy + xx
            yield rdma(mine13.at[q], got13.at[chip], s_hs.at[i, 0], r_hs.at[chip, 0], dev(z, yy, xx, c))
            yield rdma(mined.at[q], gotd.at[chip], s_hs.at[i, 1], r_hs.at[chip, 1], dev(z, yy, xx, c))

    def hot_piece(zz, q):
        ls = pl.ds(nl * zz, nl)
        return hot13.at[ls, rows13(q), :], hotd.at[ls, rowsd(q), :]

    def hot_rows(q):
        return hot13.at[:, rows13(q), :], hotd.at[:, rowsd(q), :]

    z1 = z + 1 - 2 * (z % 2)
    zc = 3 - z
    zf = 3 - z1

    def sel_local():
        p13, pd = hot_piece(z, j)
        yield pltpu.make_async_copy(sel13, p13, l_hot.at[2])
        yield pltpu.make_async_copy(seld, pd, l_hot.at[3])

    def along_z():
        p13, pd = hot_piece(z, j)
        for i, to in enumerate((zc, z1)):
            yield rdma(sel13, p13, s_hz.at[i, 0], r_hz.at[z, 0], (to, j))
            yield rdma(seld, pd, s_hz.at[i, 1], r_hz.at[z, 1], (to, j))

    def forward_z():
        p13, pd = hot_piece(zc, j)
        yield rdma(p13, p13, s_hz.at[2, 0], r_hz.at[zc, 0], (z1, j))
        yield rdma(pd, pd, s_hz.at[2, 1], r_hz.at[zc, 1], (z1, j))

    def hot_z_landed(zz):
        for a, ref in enumerate(hot_piece(zz, j)):
            landed(ref, r_hz.at[zz, a])

    def gather():
        p13, pd = hot_rows(j)
        for i, (yy, xx) in enumerate(same_core):
            yield rdma(p13, p13, s_hp.at[i, 0], r_hp.at[j, 0], dev(z, yy, xx, c))
            yield rdma(pd, pd, s_hp.at[i, 1], r_hp.at[j, 1], dev(z, yy, xx, c))
        yield rdma(p13, p13, s_hp.at[3, 0], r_hp.at[j, 0], dev(z, y, x, 1 - c))
        yield rdma(pd, pd, s_hp.at[3, 1], r_hp.at[j, 1], dev(z, y, x, 1 - c))

    def hot_rows_landed(q):
        for a, ref in enumerate(hot_rows(q)):
            landed(ref, r_hp.at[q, a])

    def to_sibling(i):
        yy, xx = same_core[i]
        q = 4 * yy + 2 * xx + c
        p13, pd = hot_rows(q)
        yield rdma(p13, p13, s_hp.at[4 + i, 0], r_hp.at[q, 0], dev(z, y, x, 1 - c))
        yield rdma(pd, pd, s_hp.at[4 + i, 1], r_hp.at[q, 1], dev(z, y, x, 1 - c))

    def build_all():
        for cp in part_loads():
            cp.wait()
        kh = lax.rem(hot_ref[0], 4)

        def build(i, carry):
            t, b = i // 4, i % 4
            for par, to13, tod in ((1 - c, give13, gived), (c, pair13.at[c], paird.at[c])):
                rr = pl.ds(pl.multiple_of((2 * b + par) * r8, r8), r8)
                rd = pl.ds(pl.multiple_of((2 * b + par) * d8, d8), d8)
                to13[b, t, :, 0:ff] = part_g[kh, t, rr, :]
                to13[b, t, :, ff:2 * ff] = part_u[kh, t, rr, :]
                tod[b, t] = part_d[kh, t, rd, :]
            return carry

        lax.fori_loop(0, nl * 4, build, 0)

    def merge():
        landed(pair13.at[1 - c], r_pair.at[0])
        landed(paird.at[1 - c], r_pair.at[1])
        core = lax.rem(hot_ref[0] // 4, 2)

        def pick(i, carry):
            b, t = i // nl, i % nl
            mine13[b, t] = pair13[core, b, t]
            mined[b, t] = paird[core, b, t]
            return carry

        lax.fori_loop(0, nl * 4, pick, 0)

    def run(group):
        for cp in group:
            cp.start()

    def select():
        for cp in scatter_local():
            cp.wait()
        for yy, xx in same_core:
            q = 2 * yy + xx
            landed(got13.at[q], r_hs.at[q, 0])
            landed(gotd.at[q], r_hs.at[q, 1])
        owner = lax.div(hot_ref[0], 8)
        sel13[...] = got13[owner]
        seld[...] = gotd[owner]

    def sct():
        run(scatter_local())
        run(scatter())

    def alongz():
        run(along_z())
        run(sel_local())

    def fwd():
        hot_z_landed(zc)
        run(forward_z())

    def gat():
        for cp in sel_local():
            cp.wait()
        hot_z_landed(z1)
        hot_z_landed(zf)
        run(gather())

    def sib():
        for i in range(3):
            yy, xx = same_core[i]
            hot_rows_landed(4 * yy + 2 * xx + c)
            run(to_sibling(i))

    steps = dict(load=lambda: run(part_loads()), build=build_all, pair=lambda: run(pair()), merge=merge, scatter=sct,
                 select=select, alongz=alongz, fwd=fwd, gather=gat, sib=sib)
    for p in range(len(CUTS[0])):
        steps[f'zf{p}'] = functools.partial(zfirst, p)
    for t in range(nl):
        steps[f'own{t}'] = functools.partial(own, t, start, start)
        for p in range(len(CUTS[t])):
            steps[f'in{t}{p}'] = functools.partial(p1, t, p, start)
            steps[f'z{t}{p}'] = functools.partial(zsend, t, p, True, start, start)
    for step in ORDER:
        steps[step]()

    for yy in range(2):
        for xx in range(2):
            hot_rows_landed(4 * yy + 2 * xx + 1 - c)
    for zz in range(4):
        for t in range(nl):
            lay = nl * zz + t
            away = z != zz
            sib = jnp.logical_and(z == zt, c != y)

            @pl.when(jnp.logical_or(away, sib))
            def _():
                landed(home13.at[lay], r_home.at[lay, 0])
                landed(homed.at[lay], r_home.at[lay, 1])

    for t in range(nl):
        own(t, wait, wait_send)
        for p in range(len(CUTS[t])):
            p1(t, p, wait_send)
            zsend(t, p, False, wait, wait_send)
    for group in (pair(), scatter(), along_z(), forward_z(), gather(), to_sibling(0), to_sibling(1), to_sibling(2)):
        for cp in group:
            cp.wait_send()


def place_kernel(slots_ref, home13, homed, hot13, hotd, w13, wd, zero13, zerod, sem):
    n = lax.axis_index('stage') * 8 + lax.axis_index('expert')
    nlay = home13.shape[0]
    step = nlay // 4

    def put(slot, src13, srcd, act):
        for i in range(0, nlay, step):
            ls = pl.ds(i, step)
            act(pltpu.make_async_copy(src13.at[ls], w13.at[ls, slot], sem.at[slot, i, 0]))
            act(pltpu.make_async_copy(srcd.at[ls], wd.at[ls, slot], sem.at[slot, i, 1]))

    start = lambda cp: cp.start()
    wait = lambda cp: cp.wait()
    put(0, home13, homed, start)
    used = [slots_ref[h, n] >= 0 for h in range(2)]
    empty = jnp.logical_not(jnp.logical_and(*used))

    for h in range(2):
        @pl.when(used[h])
        def _():
            put(1 + h, hot13, hotd, start)

    def zeros(h, act):
        for lay in range(nlay):
            act(pltpu.make_async_copy(zero13, w13.at[lay, 1 + h], sem.at[3 + h, lay, 0]))
            act(pltpu.make_async_copy(zerod, wd.at[lay, 1 + h], sem.at[3 + h, lay, 1]))

    @pl.when(empty)
    def _():
        zero13[...] = jnp.zeros_like(zero13)
        zerod[...] = jnp.zeros_like(zerod)
        for h in range(2):
            pl.when(jnp.logical_not(used[h]))(functools.partial(zeros, h, start))
        for h in range(2):
            pl.when(jnp.logical_not(used[h]))(functools.partial(zeros, h, wait))

    for h in range(2):
        @pl.when(used[h])
        def _():
            put(1 + h, hot13, hotd, wait)
    put(0, home13, homed, wait)


def solution(mesh):
    flat = ('stage', 'expert')
    any_spec = pl.BlockSpec(memory_space=pl.ANY)
    smem = pl.BlockSpec(memory_space=pltpu.SMEM)
    vmem = pl.BlockSpec(memory_space=pltpu.VMEM)

    def body(gate, up, down, hot_units, slot_map):
        nl, _, dm, f4 = gate.shape
        ff = f4 // 4
        lay = nl * 4
        r8, d8 = dm // 8, ff // 8
        cut = max(map(len, CUTS))
        dma = pltpu.SemaphoreType.DMA
        shapes = [(lay, dm, 2 * ff), (lay, ff, dm)] * 2
        outs = pl.pallas_call(
            functools.partial(exchange_kernel, (nl, dm, ff)),
            out_shape=[pltpu.VMEM(s, BF16) for s in shapes],
            in_specs=[smem, any_spec, any_spec, any_spec],
            out_specs=[vmem] * 4,
            scratch_shapes=[
                pltpu.VMEM((4, nl, dm, ff), BF16), pltpu.VMEM((4, nl, dm, ff), BF16), pltpu.VMEM((4, nl, ff, dm), BF16),
                pltpu.VMEM((2, 4, nl, r8, 2 * ff), BF16), pltpu.VMEM((2, 4, nl, d8, dm), BF16),
                pltpu.VMEM((4, nl, r8, 2 * ff), BF16), pltpu.VMEM((4, nl, d8, dm), BF16),
                pltpu.VMEM((4, nl, r8, 2 * ff), BF16), pltpu.VMEM((4, nl, d8, dm), BF16),
                pltpu.VMEM((3, nl, dm, 2 * ff), BF16), pltpu.VMEM((3, nl, ff, dm), BF16),
                pltpu.VMEM((4, nl, r8, 2 * ff), BF16), pltpu.VMEM((4, nl, d8, dm), BF16),
                pltpu.VMEM((nl, r8, 2 * ff), BF16), pltpu.VMEM((nl, d8, dm), BF16),
                dma((2, nl, 3)), dma((2, 2, nl, cut, 3)), dma((3, nl, cut, 2)), dma((2,)), dma((3, 2)), dma((3, 2)), dma((7, 2)),
                dma((3, nl, cut, 2)), dma((lay, 2)), dma((2,)), dma((4, 2)), dma((4, 2)), dma((8, 2)),
                dma((nl, 3)), dma((nl, cut, 2)), dma((4, 3)), dma((4,)),
            ],
            compiler_params=pltpu.CompilerParams(has_side_effects=True, vmem_limit_bytes=44 << 20),
            name='exchange',
        )(hot_units, gate, up, down)
        return pl.pallas_call(
            place_kernel,
            out_shape=[jax.ShapeDtypeStruct((lay, 3, dm, 2 * ff), BF16), jax.ShapeDtypeStruct((lay, 3, ff, dm), BF16)],
            in_specs=[smem] + [vmem] * 4,
            out_specs=[any_spec] * 2,
            scratch_shapes=[pltpu.VMEM((dm, 2 * ff), BF16), pltpu.VMEM((ff, dm), BF16), dma((5, lay, 2))],
            compiler_params=pltpu.CompilerParams(vmem_limit_bytes=20 << 20),
            name='place',
        )(slot_map.T, *outs)

    specs = P('stage', 'expert')
    return jax.shard_map(body, mesh=mesh, in_specs=(specs, specs, specs, P(), P()),
                         out_specs=(P(None, flat), P(None, flat)), check_vma=False)
```
